32 devices in a mesh: groups: 2 (over x), elem: 16 (over z, y, core).
Axes of the slice: x: 2, y: 2, z: 4, core: 2. Of those that a mesh axis runs over, the one named last changes fastest.
Arguments:
- snapshots: float32 [2, 4096, 16384], P(None, ('groups', 'elem')), parts along dimension 1, may hold values from -6 to 6
- delays: float32 [384, 2048], replicated, may hold values from -3 to 3
- element_order: int32 [4096], P('groups'), parts along dimension 0, may hold values from 0 to 2047, each once
- beam_table: int32 [512], P('groups'), parts along dimension 0, may hold values from 0 to 383
- band_len: int32 [8], replicated, may hold values from 1 to 4, 16 in all
Outputs:
- beams: float32 [16384, 2, 512], P('elem', None, 'groups'), parts along dimension 2
- power_db: float32 [8, 512], P(None, 'groups'), parts along dimension 1
The draws below stay inside these ranges and needn't reach their ends.
There are 2 independent parts, one for each index of `groups`. The reference program is written for one: setup_inputs(seed, part) draws one part's arguments, and reference() takes and returns one part's arrays. A program takes and returns all parts, laid end to end along the dimension named above; an argument that names none is the same for every part. Nothing has to cross between parts.
Inputs may be any that keep to these rules, and one draw needn't show every extreme that they name: `element_order`: each of 0 to 2047 appears once. `band_len`: the entries sum to 16.
All inputs are finite; a program needn't handle non-finite values.
Results may differ from the reference program's by a relative error of at most 0.0003.
Values sent between devices are 32-bit elements; how exact they have to be, the bound alone decides.
A program may use at most 128 MiB of HBM per device.

```python
import math
import jax
import jax.numpy as jnp
import numpy as np
from jax import lax

E = 2048
BEAMS = 256
DIRS = 384
BANDS = 8
UNITS = 16
BAND_MOST = 4
COLS = 16384


def place_ends(drawn, key, least, high):
    longest = drawn.shape.index(max(drawn.shape))
    spots = []
    for shift in (0, 1):
        where = [jax.random.randint(jax.random.fold_in(key, axis), (), 0, length) for axis, length in enumerate(drawn.shape)]
        where[longest] = (where[longest] + shift) % drawn.shape[longest]
        spots.append(tuple(where))
    return drawn.at[spots[0]].set(least).at[spots[1]].set(high)


def levels(key, dims, pieces, least, largest):
    factor_of, own = 1.0, jax.random.fold_in(key, 6)
    for dim, shards_of in pieces:
        draws = jnp.exp(jax.random.uniform(jax.random.fold_in(own, dim), (shards_of,), jnp.float32, least / len(pieces), largest / len(pieces)))
        factor_of = factor_of * jnp.repeat(draws, dims[dim] // shards_of).reshape([-1 if axis == dim else 1 for axis in range(len(dims))])
    return factor_of


def profile(number_of, total, limit, lean):
    loads = [(1 << 20) // math.isqrt(rank ** lean) + 1 for rank in range(2, number_of + 1)]
    rest, holding = total - limit - (number_of - 1), [1] * (number_of - 1)
    while rest > 0:
        movable = [i for i in range(number_of - 1) if holding[i] < limit]
        whole, budget = sum([loads[i] for i in movable]), rest
        for i in movable:
            more = min(limit - holding[i], max(1, budget * loads[i] // whole), rest)
            holding[i] = holding[i] + more
            rest = rest - more
    return np.array([limit] + holding)


def uneven_parts(stream_key, amount, total, most, lean):
    if amount == 2:
        one = jax.random.randint(stream_key, (), max(1, total - most), min(most, total - 1) + 1)
        return jnp.stack([one, total - one])
    sizes = jnp.asarray(profile(amount, total, most, lean), jnp.int32)
    couples = (amount - 1) // 2
    giver, taker = sizes[1:1 + 2 * couples:2], sizes[2:2 + 2 * couples:2]
    slack = jnp.minimum(giver - 1, most - taker)
    passed = jax.random.randint(jax.random.fold_in(stream_key, 1), (couples,), 0, 1 << 20) % (slack + 1)
    sizes = sizes.at[1:1 + 2 * couples:2].set(giver - passed).at[2:2 + 2 * couples:2].set(taker + passed)
    return sizes[jax.random.permutation(jax.random.fold_in(stream_key, 2), amount)]


def bell_draw(stream_key, dims, scale, most, split=(), held_as=jnp.bfloat16):
    gain = levels(stream_key, dims, split, -0.22, 0.18) if split else 1.0
    entries = jax.random.normal(stream_key, dims, jnp.float32) * scale * gain
    return jnp.minimum(jnp.maximum(entries, -most), most).astype(held_as)


def setup_inputs(seed: int = 0, part: int = 0) -> dict:
    splits = jax.random.split(jax.random.key(seed), 6)
    own_keys = jax.random.split(jax.random.fold_in(splits[5], part), 6)
    return {
        "snapshots": bell_draw(own_keys[0], (2, E, COLS), 1.0, 6.0, ((1, 16),), jnp.float32),
        "delays": jnp.clip(jax.random.uniform(splits[1], (DIRS, E), jnp.float32, -3.0, 3.0), -3.0, 3.0),
        "element_order": jax.random.permutation(own_keys[2], E).astype(jnp.int32),
        "beam_table": place_ends(jax.random.randint(own_keys[3], (BEAMS,), 0, DIRS), jax.random.fold_in(own_keys[3], 1), 0, DIRS - 1).astype(jnp.int32),
        "band_len": uneven_parts(splits[4], BANDS, UNITS, BAND_MOST, 2).astype(jnp.int32),
    }


epsilon = 1e-6


def band_of(band_len, position, unit_count):
    band_ends = jnp.cumsum(band_len).astype(jnp.int32)
    band_index = jnp.sum((band_ends <= position).astype(jnp.int32)).astype(jnp.int32)
    selector = jnp.arange(band_len.shape[0], dtype=jnp.int32) == band_index
    band_size = jnp.sum(jnp.where(selector, band_len, 0)).astype(jnp.int32)
    band_start = (jnp.sum(jnp.where(selector, band_ends, 0)).astype(jnp.int32) - band_size).astype(jnp.int32)
    frequency = (band_start.astype(jnp.float32) + 0.5 * band_size.astype(jnp.float32)) / float(unit_count)
    return frequency, band_size, selector.astype(jnp.float32)


def steering(delays, element_order, beam_table, frequency):
    delay_rows = jnp.take(delays, beam_table, axis=0)
    delay_rows = jnp.take(delay_rows, element_order, axis=1)
    phases = (2.0 * math.pi * frequency) * delay_rows
    scaling = float(delays.shape[1]) ** -0.5
    cosines = jnp.cos(phases) * scaling
    sines = -jnp.sin(phases) * scaling
    upper_rows = jnp.concatenate([cosines.T, sines.T], axis=1)
    lower_rows = jnp.concatenate([-sines.T, cosines.T], axis=1)
    return jnp.concatenate([upper_rows, lower_rows], axis=0)


def reference(snapshots, delays, element_order, beam_table, band_len):
    unit_cols = snapshots.shape[2] // UNITS
    stacked_rows = 2 * snapshots.shape[1]
    beam_count = beam_table.shape[0]

    def one_unit(position):
        frequency, band_size, selector = band_of(band_len, position, UNITS)
        weights = steering(delays, element_order, beam_table, frequency)
        window = lax.dynamic_slice_in_dim(snapshots, position * unit_cols, unit_cols, 2)
        formed = lax.dot_general(window.reshape(stacked_rows, unit_cols), weights, (((0,), (0,)), ((), ())), precision=lax.Precision.HIGHEST, preferred_element_type=jnp.float32)
        squares = jnp.sum(formed * formed, axis=0)
        power_mean = (squares[:beam_count] + squares[beam_count:]) / (band_size.astype(jnp.float32) * unit_cols)
        return formed, selector[:, None] * power_mean[None, :]

    formed_all, partials = lax.map(one_unit, jnp.arange(UNITS, dtype=jnp.int32))
    beams = formed_all.reshape(snapshots.shape[2], 2, beam_count)
    mean_power = jnp.sum(partials, axis=0)
    return beams, 10.0 * jnp.log10(mean_power + epsilon)
```

```python
import functools
import math

import jax
import jax.numpy as jnp
from jax import lax
from jax.experimental import pallas as pl
from jax.experimental.pallas import tpu as pltpu
from jax.sharding import PartitionSpec as P

epsilon = 1e-06
SIDE = 2
RING = 4


def band_of(band_len, position, unit_count):
    band_ends = jnp.cumsum(band_len)
    band_index = jnp.sum((band_ends <= position).astype(jnp.int32))
    selector = jnp.arange(band_len.shape[0], dtype=jnp.int32) == band_index
    band_size = jnp.sum(jnp.where(selector, band_len, 0))
    band_start = jnp.sum(jnp.where(selector, band_ends, 0)) - band_size
    frequency = (band_start.astype(jnp.float32) + 0.5 * band_size.astype(jnp.float32)) / float(
        unit_count
    )
    return (frequency, band_size, selector.astype(jnp.float32))


def sincos(turns):
    reduced = turns - jnp.floor(turns + 0.5)
    x = reduced * math.pi
    q = x * x
    sin_terms = [(-1.0) ** i / math.factorial(2 * i + 1) for i in range(7)]
    cos_terms = [(-1.0) ** i / math.factorial(2 * i) for i in range(8)]
    s = jnp.full_like(q, sin_terms[-1])
    for term in sin_terms[-2::-1]:
        s = s * q + term
    s = s * x
    c = jnp.full_like(q, cos_terms[-1])
    for term in cos_terms[-2::-1]:
        c = c * q + term
    return 2.0 * s * c, 1.0 - 2.0 * s * s


def split2(v):
    high = v.astype(jnp.bfloat16)
    return high, (v - high.astype(jnp.float32)).astype(jnp.bfloat16)


def split3(v):
    high = v.astype(jnp.bfloat16)
    rest = v - high.astype(jnp.float32)
    middle = rest.astype(jnp.bfloat16)
    return high, middle, (rest - middle.astype(jnp.float32)).astype(jnp.bfloat16)


def kernel(
    n, freq, x, delays, order, table, out, power,
    g1, dt, xa, xb, xz, pa, pb, ra1, ra2, rb, ry2, pw,
    own_a, own_b, sa_s, sa_r, sb_s, sb_r, sy_s, sy_r, sz_s, sz_r,
    b_s, b_r, a1_s, a1_r, a2_s, a2_r, y2_s, y2_r, p_s, p_r,
):
    me = lax.axis_index("elem")
    core = me % SIDE
    y = (me // SIDE) % SIDE
    z = me // (SIDE * SIDE)
    unit_cols = x.shape[2] // n
    quarter = unit_cols // 4
    half_cols = 2 * quarter
    beams = table.shape[0]
    scaling = float(delays.shape[1]) ** (-0.5)
    hop = (2, 3, 1, 0)

    def dev(zz, yy, cc):
        return ((zz % RING) * SIDE + yy % SIDE) * SIDE + cc % SIDE

    barrier = pltpu.get_barrier_semaphore()

    def greet(k, carry):
        pl.semaphore_signal(barrier, inc=1, device_id={"elem": (me + k) % n},
                            device_id_type=pl.DeviceIdType.MESH)
        return carry

    lax.fori_loop(1, n, greet, 0)
    pl.semaphore_wait(barrier, n - 1)

    def remote(src, dst, send, recv, target):
        return pltpu.make_async_remote_copy(
            src_ref=src, dst_ref=dst, send_sem=send, recv_sem=recv,
            device_id={"elem": target}, device_id_type=pl.DeviceIdType.MESH)

    def cols(unit, start, size):
        return x.at[:, :, pl.ds(pl.multiple_of(unit * unit_cols + start, 128), size)]

    sends = []

    def go(copy):
        copy.start()
        sends.append(copy)
        return copy

    cz = {}
    for yr in (1, 0):
        for r in (0, 1):
            for d in (0, 1):
                unit = dev(z + 2, y + yr, core + r)
                cz[d, r, yr] = go(remote(
                    cols(unit, half_cols + d * quarter, quarter), xz.at[d, r, yr],
                    sz_s.at[d, r, yr], sz_r.at[d, r, yr], dev(z + 3 - 2 * d, y, core + r)))
    cy = {}
    for j in range(4):
        for r in (0, 1):
            unit = dev(z + hop[j], y + 1, core + r)
            cy[r, j] = go(remote(
                cols(unit, 0, half_cols), xa.at[2 + r, j],
                sy_s.at[r, j], sy_r.at[r, j], dev(z, y + 1, core + r)))
    ca, cb, la, lb = {}, {}, {}, {}
    for jj in range(3):
        for yr in (1, 0):
            unit = dev(z + hop[jj + 1], y + yr, core + 1)
            cb[jj, yr] = go(remote(
                cols(unit, half_cols, half_cols), xb.at[1, jj, yr],
                sb_s.at[jj, yr], sb_r.at[jj, yr], dev(z, y, core + 1)))
            lb[jj, yr] = pltpu.make_async_copy(
                cols(dev(z + hop[jj + 1], y + yr, core), half_cols, half_cols),
                xb.at[0, jj, yr], own_b.at[jj, yr])
            lb[jj, yr].start()
    for j in range(4):
        ca[j] = go(remote(
            cols(dev(z + hop[j], y, core + 1), 0, half_cols), xa.at[1, j],
            sa_s.at[j], sa_r.at[j], dev(z, y, core + 1)))
        la[j] = pltpu.make_async_copy(
            cols(dev(z + hop[j], y, core), 0, half_cols), xa.at[0, j], own_a.at[j])
        la[j].start()

    beam_hot = jnp.where(
        lax.broadcasted_iota(jnp.int32, (beams, delays.shape[0]), 1) == table[...], 1.0, 0.0
    ).astype(jnp.bfloat16)
    step = 512 if delays.shape[1] % 512 == 0 else delays.shape[1]

    def pick_beams(i, carry):
        span = pl.ds(pl.multiple_of(i * step, step), step)
        parts = split3(delays[:, span])
        rows = [jnp.dot(beam_hot, part, preferred_element_type=jnp.float32) for part in parts]
        for m, part in enumerate(rows):
            g1[m * beams:(m + 1) * beams, span] = part.astype(jnp.bfloat16)
        return carry

    lax.fori_loop(0, delays.shape[1] // step, pick_beams, 0)

    def pick_elems(s, carry):
        r, g = s % 2, s // 2
        q = dev(z + (g // 2) * (1 + 2 * (g % 2)), y + (g % 2) * (1 - g // 2), core + r)
        row = order[q]
        hot = jnp.where(
            lax.broadcasted_iota(jnp.int32, (delays.shape[1], row.shape[1]), 0) == row, 1.0, 0.0
        ).astype(jnp.bfloat16)
        got = jnp.dot(g1[...], hot, preferred_element_type=jnp.float32)
        dt[s] = got[:beams] + got[beams:2 * beams] + got[2 * beams:]
        return carry

    lax.fori_loop(0, 8, pick_elems, 0)

    def term(xv, s, f):
        sine, cosine = sincos(f * dt[s])
        ch, cl = split2(cosine * scaling)
        sh, sl = split2(sine * scaling)
        wh = jnp.concatenate(
            [jnp.concatenate([ch, sh], axis=1), jnp.concatenate([-sh, ch], axis=1)], axis=0)
        wl = jnp.concatenate(
            [jnp.concatenate([cl, sl], axis=1), jnp.concatenate([-sl, cl], axis=1)], axis=0)
        xh, xl = split2(xv.reshape(xv.shape[0] * xv.shape[1], xv.shape[2]))
        dot = functools.partial(jnp.dot, preferred_element_type=jnp.float32)
        return dot(wh, xh) + (dot(wh, xl) + dot(wl, xh))

    def part(h):
        return pl.ds(pl.multiple_of(h * quarter, 128), quarter)

    def chip_terms(jj, yr, h, f):
        pb[jj, yr, h] = term(xb[0, jj, yr, :, :, part(h)], 0, f)

        def add(s, carry):
            pb[jj, yr, h] += term(xb[s, jj, yr, :, :, part(h)], s, f)
            return carry

        lax.fori_loop(1, 2, add, 0)

    def b_copy(jj, yr, h):
        return remote(pb.at[jj, yr, h], rb.at[jj, yr, h], b_s.at[jj, yr, h], b_r.at[jj, yr, h],
                      dev(z + 3 - 2 * jj, y, core))

    def b_freq(jj, yr):
        return freq[dev(z + 3 - 2 * jj, y + yr, core)]

    for jj in (0, 1):
        for yr in (1, 0):
            lb[jj, yr].wait()
            cb[jj, yr].wait_recv()

    def b_alone(t, carry):
        jj, yr = t % 2, 1 - t // 2
        chip_terms(jj, yr, 1 - jj, b_freq(jj, yr))
        b_copy(jj, yr, 1 - jj).start()
        return carry

    lax.fori_loop(0, 4, b_alone, 0)
    for yr in (1, 0):
        for r in (0, 1):
            for d in (0, 1):
                cz[d, r, yr].wait_recv()

    def b_joint(t, carry):
        jj, yr = t % 2, 1 - t // 2
        f = b_freq(jj, yr)
        chip_terms(jj, yr, jj, f)

        def add(r, inner):
            pb[jj, yr, jj] += term(xz[jj, r, yr], 4 + 2 * jj + r, f)
            return inner

        lax.fori_loop(0, 2, add, 0)
        b_copy(jj, yr, jj).start()
        return carry

    lax.fori_loop(0, 4, b_joint, 0)

    def a_slot(j):
        la[j].wait()
        ca[j].wait_recv()
        for r in (0, 1):
            cy[r, j].wait_recv()
        f = freq[dev(z + hop[j], y, core)]
        for h in (0, 1):
            pa[j, h] = jnp.zeros_like(pa[j, h])

        def add(t, carry):
            h, s = t % 2, t // 2
            pa[j, h] += term(xa[s, j, :, :, part(h)], s, f)
            return carry

        lax.fori_loop(0, 8, add, 0)

    a_slot(0)
    ca1 = [go(remote(pa.at[0, h], ra1.at[h], a1_s.at[h], a1_r.at[h], dev(z + 3 - 2 * h, y, core)))
           for h in (0, 1)]

    for yr in (1, 0):
        lb[2, yr].wait()
        cb[2, yr].wait_recv()

    def b_own(t, carry):
        yr, h = t % 2, t // 2
        chip_terms(2, yr, h, freq[dev(z, y + yr, core)])
        return carry

    lax.fori_loop(0, 4, b_own, 0)

    ca2 = {}

    def a_send(d, h):
        ca2[d, h] = go(remote(pa.at[1 + d, h], ra2.at[d, h], a2_s.at[d, h], a2_r.at[d, h],
                              dev(z + 3 - 2 * d, y, core)))

    def a_joint(d):
        ca1[d].wait_recv()
        pa[1 + d, d] += ra1[d]
        a_send(d, d)

    a_slot(1)
    a_send(0, 1)
    a_joint(0)
    a_slot(2)
    a_send(1, 0)
    a_joint(1)

    def b_gather(yr):
        for h in (0, 1):
            for jj in (0, 1):
                b_copy(jj, yr, h).wait_recv()
            pb[2, yr, h] += rb[0, yr, h] + rb[1, yr, h]

    cy2 = []
    b_gather(1)
    for h in (0, 1):
        cy2.append(go(remote(pb.at[2, 1, h], ry2.at[h], y2_s.at[h], y2_r.at[h],
                             dev(z, y + 1, core))))
    b_gather(0)
    a_slot(3)

    for h in (0, 1):
        for d in (0, 1):
            ca2[d, h].wait_recv()
        got = (pa[3, h] + ra2[0, h] + ra2[1, h]).T
        out[h * quarter:(h + 1) * quarter, :] = got
        squares = jnp.sum(got * got, axis=0, keepdims=True)
        total = squares if h == 0 else total + squares
    for h in (0, 1):
        cy2[h].wait_recv()
        got = (pb[2, 0, h] + ry2[h]).T
        out[half_cols + h * quarter:half_cols + (h + 1) * quarter, :] = got
        total = total + jnp.sum(got * got, axis=0, keepdims=True)
    both = total[:, :beams] + total[:, beams:]
    pw[0] = jnp.broadcast_to(both, pw.shape[1:])

    def p_copy(k):
        return remote(pw.at[0], pw.at[k], p_s.at[k], p_r.at[k], (me + k) % n)

    def p_start(k, carry):
        p_copy(k).start()
        return carry

    def p_wait(k, carry):
        p_copy(k).wait()
        return carry

    lax.fori_loop(1, n, p_start, 0)
    for copy in sends:
        copy.wait_send()

    def b_drain(t, carry):
        b_copy(t // 4, (t // 2) % 2, t % 2).wait_send()
        return carry

    lax.fori_loop(0, 8, b_drain, 0)
    lax.fori_loop(1, n, p_wait, 0)
    power[...] = pw[...]


def local_ring(n, snapshots, delays, element_order, beam_table, band_len):
    local_elems = snapshots.shape[1]
    unit_cols = snapshots.shape[2] // n
    beams = beam_table.shape[0]
    half_cols, quarter = unit_cols // 2, unit_cols // 4
    units = jnp.arange(n, dtype=jnp.int32)
    frequency, band_size, selector = jax.vmap(lambda u: band_of(band_len, u, n))(units)
    f32, sem = jnp.float32, pltpu.SemaphoreType.DMA
    raw = (2, local_elems)
    vmem, hbm, smem = (pl.BlockSpec(memory_space=m) for m in (pltpu.VMEM, pl.ANY, pltpu.SMEM))
    formed, power = pl.pallas_call(
        functools.partial(kernel, n),
        out_shape=(
            jax.ShapeDtypeStruct((unit_cols, 2 * beams), f32),
            jax.ShapeDtypeStruct((n, 8, beams), f32),
        ),
        in_specs=[smem, hbm, vmem, vmem, vmem],
        out_specs=(vmem, vmem),
        scratch_shapes=[
            pltpu.VMEM((3 * beams, delays.shape[1]), jnp.bfloat16),
            pltpu.VMEM((8, beams, local_elems), f32),
            pltpu.VMEM((4, 4) + raw + (half_cols,), f32),
            pltpu.VMEM((2, 3, 2) + raw + (half_cols,), f32),
            pltpu.VMEM((2, 2, 2) + raw + (quarter,), f32),
            pltpu.VMEM((4, 2, 2 * beams, quarter), f32),
            pltpu.VMEM((3, 2, 2, 2 * beams, quarter), f32),
            pltpu.VMEM((2, 2 * beams, quarter), f32),
            pltpu.VMEM((2, 2, 2 * beams, quarter), f32),
            pltpu.VMEM((2, 2, 2, 2 * beams, quarter), f32),
            pltpu.VMEM((2, 2 * beams, quarter), f32),
            pltpu.VMEM((n, 8, beams), f32),
            sem((4,)), sem((3, 2)),
            sem((4,)), sem((4,)), sem((3, 2)), sem((3, 2)),
            sem((2, 4)), sem((2, 4)), sem((2, 2, 2)), sem((2, 2, 2)),
            sem((2, 2, 2)), sem((2, 2, 2)), sem((2,)), sem((2,)),
            sem((2, 2)), sem((2, 2)), sem((2,)), sem((2,)),
            sem((n,)), sem((n,)),
        ],
        compiler_params=pltpu.CompilerParams(
            collective_id=0, has_side_effects=True, vmem_limit_bytes=62 * 1024 * 1024
        ),
    )(
        frequency, snapshots, delays,
        element_order.reshape(n, 1, local_elems), beam_table.reshape(beams, 1),
    )
    row_unit = (lax.axis_index("elem") + n - units) % n
    share = selector / (band_size.astype(f32) * unit_cols)[:, None]
    summed = jnp.sum(share[row_unit][:, :, None] * power[:, 0][:, None, :], axis=0)
    decibels = 10.0 * jnp.log10(summed + epsilon)
    return (formed.reshape(unit_cols, 2, beams), decibels)


def fits(mesh):
    return mesh.shape["elem"] == SIDE * SIDE * RING


def steering(delays, element_order, beam_table, frequency):
    delay_rows = jnp.take(delays, beam_table, axis=0)
    delay_rows = jnp.take(delay_rows, element_order, axis=1)
    phases = 2.0 * math.pi * frequency * delay_rows
    scaling = float(delays.shape[1]) ** (-0.5)
    cosines = jnp.cos(phases) * scaling
    sines = -jnp.sin(phases) * scaling
    upper_rows = jnp.concatenate([cosines.T, sines.T], axis=1)
    lower_rows = jnp.concatenate([-sines.T, cosines.T], axis=1)
    return jnp.concatenate([upper_rows, lower_rows], axis=0)


def project(arrived, weights):
    columns = arrived.shape[2]
    stacked = arrived.reshape(2 * arrived.shape[1], columns)
    return lax.dot_general(
        stacked,
        weights,
        (((0,), (0,)), ((), ())),
        precision=lax.Precision.HIGHEST,
        preferred_element_type=jnp.float32,
    )


def local(snapshots, delays, element_order, beam_table, band_len):
    unit_count = lax.axis_size("elem")
    position = lax.axis_index("elem")
    frequency, band_size, selector = band_of(band_len, position, unit_count)
    weights = steering(delays, element_order, beam_table, frequency)
    beam_count = beam_table.shape[0]
    local_elems = snapshots.shape[1]
    unit_cols = snapshots.shape[2] // unit_count
    divided = snapshots.reshape(2, local_elems, unit_count, unit_cols)
    pieces = lax.all_to_all(divided, "elem", split_axis=2, concat_axis=1, tiled=True)
    formed = project(pieces.reshape(2, pieces.shape[1], pieces.shape[3]), weights)
    column_count = formed.shape[0]
    squares = jnp.sum(formed * formed, axis=0)
    power_mean = (squares[:beam_count] + squares[beam_count:]) / (
        band_size.astype(jnp.float32) * column_count
    )
    partial_value = selector[:, None] * power_mean[None, :]
    summed = lax.psum(partial_value, "elem")
    decibels = 10.0 * jnp.log10(summed + epsilon)
    return (formed.reshape(column_count, 2, beam_count), decibels)


def solution(mesh):
    n = mesh.shape["elem"]
    body = functools.partial(local_ring, n) if fits(mesh) else local
    return jax.shard_map(
        body,
        mesh=mesh,
        in_specs=(P(None, ("groups", "elem"), None), P(), P("groups"), P("groups"), P()),
        out_specs=(P("elem", None, "groups"), P(None, "groups")),
        check_vma=False,
    )
```

```python
import functools
import math

import jax
import jax.numpy as jnp
from jax import lax
from jax.experimental import pallas as pl
from jax.experimental.pallas import tpu as pltpu
from jax.sharding import PartitionSpec as P

epsilon = 1e-06
SIDE = 2
RING = 4
CHUNKS = 8


def band_of(band_len, position, unit_count):
    band_ends = jnp.cumsum(band_len)
    band_index = jnp.sum((band_ends <= position).astype(jnp.int32))
    selector = jnp.arange(band_len.shape[0], dtype=jnp.int32) == band_index
    band_size = jnp.sum(jnp.where(selector, band_len, 0))
    band_start = jnp.sum(jnp.where(selector, band_ends, 0)) - band_size
    frequency = (band_start.astype(jnp.float32) + 0.5 * band_size.astype(jnp.float32)) / float(
        unit_count
    )
    return (frequency, band_size, selector.astype(jnp.float32))


def sincos(turns):
    reduced = turns - jnp.floor(turns + 0.5)
    x = reduced * math.pi
    q = x * x
    sin_terms = [(-1.0) ** i / math.factorial(2 * i + 1) for i in range(7)]
    cos_terms = [(-1.0) ** i / math.factorial(2 * i) for i in range(8)]
    s = jnp.full_like(q, sin_terms[-1])
    for term in sin_terms[-2::-1]:
        s = s * q + term
    s = s * x
    c = jnp.full_like(q, cos_terms[-1])
    for term in cos_terms[-2::-1]:
        c = c * q + term
    return 2.0 * s * c, 1.0 - 2.0 * s * s


def split2(v):
    high = v.astype(jnp.bfloat16)
    return high, (v - high.astype(jnp.float32)).astype(jnp.bfloat16)


def split3(v):
    high = v.astype(jnp.bfloat16)
    rest = v - high.astype(jnp.float32)
    middle = rest.astype(jnp.bfloat16)
    return high, middle, (rest - middle.astype(jnp.float32)).astype(jnp.bfloat16)


def kernel(
    n, freq, x, delays, order, table, out, power,
    g1, dt, wh, wl, xa, xb, xz, pa, pb, ra, rb, ry2, pw, tot,
    own_a, own_b, sa_s, sa_r, sb_s, sb_r, sy_s, sy_r, sz_s, sz_r,
    a_s, a_r, b_s, b_r, y2_s, y2_r, p_s, p_r,
):
    me = lax.axis_index("elem")
    core = me % SIDE
    y = (me // SIDE) % SIDE
    z = me // (SIDE * SIDE)
    upper = z // 2
    end = z + upper * (RING - 1 - 2 * z)
    unit_cols = x.shape[2] // n
    chunk = unit_cols // CHUNKS
    early = CHUNKS - 1
    early_cols = early * chunk
    beams = table.shape[0]
    scaling = float(delays.shape[1]) ** (-0.5)
    slots = (3, 2, 1 - end, end)

    def chip(u):
        return u + upper * (RING - 1 - 2 * u)

    def dev(zz, yy, cc):
        return (zz * SIDE + yy % SIDE) * SIDE + cc % SIDE

    ahead = dev(chip(end + 1), y, core)
    beside = dev(chip(1 - end), y, core)

    barrier = pltpu.get_barrier_semaphore()

    def greet(k, carry):
        pl.semaphore_signal(barrier, inc=1, device_id={"elem": (me + k) % n},
                            device_id_type=pl.DeviceIdType.MESH)
        return carry

    lax.fori_loop(1, n, greet, 0)
    pl.semaphore_wait(barrier, n - 1)

    def remote(src, dst, send, recv, target):
        return pltpu.make_async_remote_copy(
            src_ref=src, dst_ref=dst, send_sem=send, recv_sem=recv,
            device_id={"elem": target}, device_id_type=pl.DeviceIdType.MESH)

    def cols(unit, start, size):
        return x.at[:, :, pl.ds(pl.multiple_of(unit * unit_cols + start, 128), size)]

    def part(k):
        return pl.ds(pl.multiple_of(k * chunk, 128), chunk)

    def y_copy(j, k, r):
        return remote(
            cols(dev(chip(slots[j]), y + 1, core + r), k * chunk, chunk),
            xa.at[2 + r, j, :, :, part(k)],
            sy_s.at[r, j, k], sy_r.at[r, j, k], dev(z, y + 1, core + r))

    def z_copy(j, yr, r):
        return remote(
            cols(dev(chip(3 - j), y + yr, core + r), early_cols, chunk), xz.at[j, r, yr],
            sz_s.at[j, r, yr], sz_r.at[j, r, yr], dev(chip(1 - end), y, core + r))

    def a_copy(j, k):
        to = j + 3 * end if j < 2 else 2
        return remote(pa.at[j, k], ra.at[to, k], a_s.at[j, k], a_r.at[to, k],
                      ahead if j < 2 else beside)

    def a_wait(to, k):
        remote(pa.at[0, k], ra.at[to, k], a_s.at[0, k], a_r.at[to, k], beside).wait_recv()

    def b_copy(j, yr):
        return remote(pb.at[j, yr], rb.at[j, yr], b_s.at[j, yr], b_r.at[j, yr],
                      ahead if j < 2 else beside)

    everyone = [(yr, j, r) for j in range(3) for yr in (1, 0) for r in (0, 1)]

    @pl.when(end == 0)
    def _():
        for yr, j, r in everyone:
            z_copy(j, yr, r).start()

    for j in range(4):
        def y_start(k, carry, j=j):
            for r in (0, 1):
                y_copy(j, k, r).start()
            return carry

        lax.fori_loop(0, early, y_start, 0)

    ca, cb, la, lb = {}, {}, {}, {}
    for j in range(4):
        there = dev(chip(slots[j]), y, core + 1)
        here = dev(chip(slots[j]), y, core)
        ca[j] = remote(cols(there, 0, early_cols), xa.at[1, j],
                       sa_s.at[j], sa_r.at[j], dev(z, y, core + 1))
        la[j] = pltpu.make_async_copy(cols(here, 0, early_cols), xa.at[0, j], own_a.at[j])
        ca[j].start()
        la[j].start()
        if j > 0:
            continue
        for i in range(4):
            for yr in (1, 0):
                there = dev(chip(slots[i]), y + yr, core + 1)
                here = dev(chip(slots[i]), y + yr, core)
                cb[i, yr] = remote(cols(there, early_cols, chunk), xb.at[1, i, yr],
                                   sb_s.at[i, yr], sb_r.at[i, yr], dev(z, y, core + 1))
                lb[i, yr] = pltpu.make_async_copy(
                    cols(here, early_cols, chunk), xb.at[0, i, yr], own_b.at[i, yr])
                cb[i, yr].start()
                lb[i, yr].start()

    beam_hot = jnp.where(
        lax.broadcasted_iota(jnp.int32, (beams, delays.shape[0]), 1) == table[...], 1.0, 0.0
    ).astype(jnp.bfloat16)
    step = 512 if delays.shape[1] % 512 == 0 else delays.shape[1]

    def pick_beams(i, carry):
        span = pl.ds(pl.multiple_of(i * step, step), step)
        parts = split3(delays[:, span])
        rows = [jnp.dot(beam_hot, piece, preferred_element_type=jnp.float32) for piece in parts]
        for m, piece in enumerate(rows):
            g1[m * beams:(m + 1) * beams, span] = piece.astype(jnp.bfloat16)
        return carry

    lax.fori_loop(0, delays.shape[1] // step, pick_beams, 0)

    def pick_elems(s, carry):
        r, g = s % 2, s // 2
        u = end + (g // 2) * (1 - 2 * end)
        q = dev(chip(u), y + g % 2, core + r)
        row = order[q]
        hot = jnp.where(
            lax.broadcasted_iota(jnp.int32, (delays.shape[1], row.shape[1]), 0) == row, 1.0, 0.0
        ).astype(jnp.bfloat16)
        got = jnp.dot(g1[...], hot, preferred_element_type=jnp.float32)
        dt[s] = got[:beams] + got[beams:2 * beams] + got[2 * beams:]
        return carry

    lax.fori_loop(0, 6, pick_elems, 0)
    wide = 2 * x.shape[1]

    def weigh(f, sources):
        for i, s in enumerate(sources):
            sine, cosine = sincos(f * dt[s])
            ch, cl = split2(cosine * scaling)
            sh, sl = split2(sine * scaling)
            span = slice(i * wide, (i + 1) * wide)
            wh[:beams, span] = jnp.concatenate([ch, sh], axis=1)
            wh[beams:, span] = jnp.concatenate([-sh, ch], axis=1)
            wl[:beams, span] = jnp.concatenate([cl, sl], axis=1)
            wl[beams:, span] = jnp.concatenate([-sl, cl], axis=1)

    def form(pieces):
        rows = jnp.concatenate([piece.reshape(wide, chunk) for piece in pieces], axis=0)
        xh, xl = split2(rows)
        span = slice(0, wide * len(pieces))
        dot = functools.partial(jnp.dot, preferred_element_type=jnp.float32)
        high = wh[:, span]
        return dot(high, xh) + (dot(high, xl) + dot(wl[:, span], xh))

    def a_slot(j, then):
        weigh(freq[dev(chip(slots[j]), y, core)], (0, 1, 2, 3))
        la[j].wait()
        ca[j].wait_recv()

        def one(k, carry):
            for r in (0, 1):
                y_copy(j, k, r).wait_recv()
            pa[j, k] = form([xa[s, j, :, :, part(k)] for s in range(4)])
            then(k)
            return carry

        lax.fori_loop(0, early, one, 0)

    def join(j, to, k):
        a_wait(to, k)
        pa[j, k] += ra[to, k]

    def after0(k):
        @pl.when(end == 0)
        def _():
            a_copy(0, k).start()

    def after1(k):
        @pl.when(end == 0)
        def _():
            a_copy(1, k).start()

        @pl.when(end == 1)
        def _():
            join(0, 0, k)
            a_copy(0, k).start()

    def after2(k):
        @pl.when(end == 1)
        def _():
            join(2, 3, k)

        a_copy(2, k).start()

        @pl.when(end == 1)
        def _():
            join(1, 1, k)
            a_copy(1, k).start()

    def emit(got, start):
        out[pl.ds(pl.multiple_of(start, 128), chunk), :] = got
        tot[...] += jnp.sum(got * got, axis=0, keepdims=True)

    def after3(k):
        @pl.when(end == 1)
        def _():
            join(3, 4, k)

        a_wait(2, k)
        emit((pa[3, k] + ra[2, k]).T, k * chunk)

    tot[...] = jnp.zeros_like(tot)
    a_slot(0, after0)

    for i in range(4):
        for yr in (1, 0):
            lb[i, yr].wait()
            cb[i, yr].wait_recv()

    @pl.when(end == 1)
    def _():
        for yr, j, r in everyone:
            z_copy(j, yr, r).wait_recv()

        def b_joint(t, carry):
            i, yr = t // 2, 1 - t % 2
            j = i + i // 2
            weigh(freq[dev(chip(3 - i), y + yr, core)], (0, 1, 4, 5))
            pb[j, yr] = form([xb[0, j, yr], xb[1, j, yr], xz[i, 0, yr], xz[i, 1, yr]])
            return carry

        lax.fori_loop(0, 6, b_joint, 0)
        for j in (0, 1):
            for yr in (1, 0):
                b_copy(j, yr).start()

    def b_end(t, carry):
        yr = 1 - t
        weigh(freq[dev(chip(0), y + yr, core)], (0, 1))
        pb[3 - end, yr] = form([xb[0, 3 - end, yr], xb[1, 3 - end, yr]])
        return carry

    lax.fori_loop(0, 2, b_end, 0)
    a_slot(1, after1)

    @pl.when(end == 1)
    def _():
        for yr in (1, 0):
            b_copy(0, yr).wait_recv()
            pb[2, yr] += rb[0, yr]
            b_copy(2, yr).start()
        for yr in (1, 0):
            b_copy(1, yr).wait_recv()
            pb[3, yr] += rb[1, yr]

    a_slot(2, after2)

    @pl.when(end == 0)
    def _():
        for yr in (1, 0):
            b_copy(2, yr).wait_recv()
            pb[3, yr] += rb[2, yr]

    last = remote(pb.at[3, 1], ry2, y2_s, y2_r, dev(z, y + 1, core))
    last.start()
    a_slot(3, after3)
    last.wait_recv()
    emit((pb[3, 0] + ry2[...]).T, early_cols)
    both = tot[:, :beams] + tot[:, beams:]
    pw[0] = jnp.broadcast_to(both, pw.shape[1:])

    def p_copy(k):
        return remote(pw.at[0], pw.at[k], p_s.at[k], p_r.at[k], (me + k) % n)

    def p_start(k, carry):
        p_copy(k).start()
        return carry

    def p_wait(k, carry):
        p_copy(k).wait()
        return carry

    lax.fori_loop(1, n, p_start, 0)
    last.wait_send()
    for j in range(4):
        ca[j].wait_send()
        for yr in (1, 0):
            cb[j, yr].wait_send()

        def drain(k, carry, j=j):
            for r in (0, 1):
                y_copy(j, k, r).wait_send()
            if j < 3:
                a_copy(j, k).wait_send()
            return carry

        lax.fori_loop(0, early, drain, 0)

    @pl.when(end == 0)
    def _():
        for yr, j, r in everyone:
            z_copy(j, yr, r).wait_send()

    @pl.when(end == 1)
    def _():
        for j in range(3):
            for yr in (1, 0):
                b_copy(j, yr).wait_send()

    lax.fori_loop(1, n, p_wait, 0)
    power[...] = pw[...]


def local_ring(n, snapshots, delays, element_order, beam_table, band_len):
    local_elems = snapshots.shape[1]
    unit_cols = snapshots.shape[2] // n
    beams = beam_table.shape[0]
    early, chunk = CHUNKS - 1, unit_cols // CHUNKS
    block = (2 * beams, chunk)
    units = jnp.arange(n, dtype=jnp.int32)
    frequency, band_size, selector = jax.vmap(lambda u: band_of(band_len, u, n))(units)
    f32, sem = jnp.float32, pltpu.SemaphoreType.DMA
    raw = (2, local_elems)
    vmem, hbm, smem = (pl.BlockSpec(memory_space=m) for m in (pltpu.VMEM, pl.ANY, pltpu.SMEM))
    formed, power = pl.pallas_call(
        functools.partial(kernel, n),
        out_shape=(
            jax.ShapeDtypeStruct((unit_cols, 2 * beams), f32),
            jax.ShapeDtypeStruct((n, 8, beams), f32),
        ),
        in_specs=[smem, hbm, vmem, vmem, vmem],
        out_specs=(vmem, vmem),
        scratch_shapes=[
            pltpu.VMEM((3 * beams, delays.shape[1]), jnp.bfloat16),
            pltpu.VMEM((6, beams, local_elems), f32),
            pltpu.VMEM((2 * beams, 8 * local_elems), jnp.bfloat16),
            pltpu.VMEM((2 * beams, 8 * local_elems), jnp.bfloat16),
            pltpu.VMEM((4, 4) + raw + (early * chunk,), f32),
            pltpu.VMEM((2, 4, 2) + raw + (chunk,), f32),
            pltpu.VMEM((3, 2, 2) + raw + (chunk,), f32),
            pltpu.VMEM((4, early) + block, f32),
            pltpu.VMEM((4, 2) + block, f32),
            pltpu.VMEM((5, early) + block, f32),
            pltpu.VMEM((3, 2) + block, f32),
            pltpu.VMEM(block, f32),
            pltpu.VMEM((n, 8, beams), f32),
            pltpu.VMEM((1, 2 * beams), f32),
            sem((4,)), sem((4, 2)),
            sem((4,)), sem((4,)), sem((4, 2)), sem((4, 2)),
            sem((2, 4, early)), sem((2, 4, early)), sem((3, 2, 2)), sem((3, 2, 2)),
            sem((3, early)), sem((5, early)), sem((3, 2)), sem((3, 2)),
            sem, sem,
            sem((n,)), sem((n,)),
        ],
        compiler_params=pltpu.CompilerParams(
            collective_id=0, has_side_effects=True, vmem_limit_bytes=62 * 1024 * 1024
        ),
    )(
        frequency, snapshots, delays,
        element_order.reshape(n, 1, local_elems), beam_table.reshape(beams, 1),
    )
    row_unit = (lax.axis_index("elem") + n - units) % n
    share = selector / (band_size.astype(f32) * unit_cols)[:, None]
    summed = jnp.sum(share[row_unit][:, :, None] * power[:, 0][:, None, :], axis=0)
    decibels = 10.0 * jnp.log10(summed + epsilon)
    return (formed.reshape(unit_cols, 2, beams), decibels)


def fits(mesh):
    return mesh.shape["elem"] == SIDE * SIDE * RING


def steering(delays, element_order, beam_table, frequency):
    delay_rows = jnp.take(delays, beam_table, axis=0)
    delay_rows = jnp.take(delay_rows, element_order, axis=1)
    phases = 2.0 * math.pi * frequency * delay_rows
    scaling = float(delays.shape[1]) ** (-0.5)
    cosines = jnp.cos(phases) * scaling
    sines = -jnp.sin(phases) * scaling
    upper_rows = jnp.concatenate([cosines.T, sines.T], axis=1)
    lower_rows = jnp.concatenate([-sines.T, cosines.T], axis=1)
    return jnp.concatenate([upper_rows, lower_rows], axis=0)


def project(arrived, weights):
    columns = arrived.shape[2]
    stacked = arrived.reshape(2 * arrived.shape[1], columns)
    return lax.dot_general(
        stacked,
        weights,
        (((0,), (0,)), ((), ())),
        precision=lax.Precision.HIGHEST,
        preferred_element_type=jnp.float32,
    )


def local(snapshots, delays, element_order, beam_table, band_len):
    unit_count = lax.axis_size("elem")
    position = lax.axis_index("elem")
    frequency, band_size, selector = band_of(band_len, position, unit_count)
    weights = steering(delays, element_order, beam_table, frequency)
    beam_count = beam_table.shape[0]
    local_elems = snapshots.shape[1]
    unit_cols = snapshots.shape[2] // unit_count
    divided = snapshots.reshape(2, local_elems, unit_count, unit_cols)
    pieces = lax.all_to_all(divided, "elem", split_axis=2, concat_axis=1, tiled=True)
    formed = project(pieces.reshape(2, pieces.shape[1], pieces.shape[3]), weights)
    column_count = formed.shape[0]
    squares = jnp.sum(formed * formed, axis=0)
    power_mean = (squares[:beam_count] + squares[beam_count:]) / (
        band_size.astype(jnp.float32) * column_count
    )
    partial_value = selector[:, None] * power_mean[None, :]
    summed = lax.psum(partial_value, "elem")
    decibels = 10.0 * jnp.log10(summed + epsilon)
    return (formed.reshape(column_count, 2, beam_count), decibels)


def solution(mesh):
    n = mesh.shape["elem"]
    body = functools.partial(local_ring, n) if fits(mesh) else local
    return jax.shard_map(
        body,
        mesh=mesh,
        in_specs=(P(None, ("groups", "elem"), None), P(), P("groups"), P("groups"), P()),
        out_specs=(P("elem", None, "groups"), P(None, "groups")),
        check_vma=False,
    )
```
